8 devices in a mesh: dp: 1 (over z), cz: 2 (over y), cy: 2 (over x), cx: 2 (over core).
Axes of the slice: x: 2, y: 2, z: 1, core: 2. Of those that a mesh axis runs over, the one named last changes fastest.
Arguments:
- x_tokens: bfloat16 [4096, 8192], P(('dp', 'cx', 'cz'), 'cy')
- w_up: bfloat16 [8192, 28672], P('cy', ('cz', 'cx'))
- w_down: bfloat16 [28672, 8192], P('cz', ('cy', 'cx'))
Outputs:
- output: bfloat16 [4096, 8192], P(('dp', 'cx', 'cz'), 'cy')
All inputs are finite; a program needn't handle non-finite values.
Results may differ from the reference program's by a relative error of at most 0.0114981.
Values are sent between devices in bfloat16 or wider.
A program may use at most 1 GiB of HBM per device.

```python
import jax
import jax.numpy as jnp
from jax import lax

MODEL_DIM = 8192
HIDDEN_DIM = 28672
TOKENS_DEV = 512
CUBE_DEVS = 8

NUM_TOKENS = TOKENS_DEV * CUBE_DEVS


def setup_inputs(seed: int = 0, part: int = 0) -> dict:
    base_key = jax.random.key(seed)
    key_x, key_up, key_down = jax.random.split(base_key, 3)
    key_x = jax.random.fold_in(key_x, part)
    x_tokens = jax.random.normal(key_x, (NUM_TOKENS, MODEL_DIM), jnp.float32)
    w_up = jax.random.normal(key_up, (MODEL_DIM, HIDDEN_DIM), jnp.float32) * MODEL_DIM ** -0.5
    w_down = jax.random.normal(key_down, (HIDDEN_DIM, MODEL_DIM), jnp.float32) * HIDDEN_DIM ** -0.5
    return {'x_tokens': x_tokens.astype(jnp.bfloat16), 'w_up': w_up.astype(jnp.bfloat16), 'w_down': w_down.astype(jnp.bfloat16)}


def mlp_block(row_block, w_up, w_down):
    pre_act = jnp.dot(row_block, w_up, preferred_element_type=jnp.float32).astype(jnp.bfloat16)
    hidden = jax.nn.gelu(pre_act.astype(jnp.float32), approximate=True).astype(jnp.bfloat16)
    return jnp.dot(hidden, w_down, preferred_element_type=jnp.float32).astype(jnp.bfloat16)


def reference(x_tokens, w_up, w_down):
    row_blocks = x_tokens.reshape(CUBE_DEVS, TOKENS_DEV, MODEL_DIM)
    out_blocks = lax.map(lambda row_block: mlp_block(row_block, w_up, w_down), row_blocks)
    return out_blocks.reshape(NUM_TOKENS, MODEL_DIM)
```

```python
import jax
import jax.numpy as jnp
from jax import lax
from jax.sharding import PartitionSpec as P


CHUNKS = (2, 2, 2, 1)
B_BLOCKS = (2, 2)
A_BLOCKS = (2, 1, 1)


def solution(mesh):
    data_spec = P(('dp', 'cx', 'cz'), 'cy')
    up_spec = P('cy', ('cz', 'cx'))
    down_spec = P('cz', ('cy', 'cx'))
    swap = [(0, 1), (1, 0)]

    def to_core(v):
        return lax.ppermute(v, 'cx', swap)

    def to_y(v):
        return lax.ppermute(v, 'cz', swap)

    def to_x(v):
        return lax.ppermute(v, 'cy', swap)

    def to_diag(v):
        return lax.ppermute(v, ('cy', 'cx'), [(0, 3), (1, 2), (2, 1), (3, 0)])

    def after(v, *deps):
        return lax.optimization_barrier((v, *deps))[0]

    def cat(pieces, axis):
        return pieces[0] if len(pieces) == 1 else jnp.concatenate(pieces, axis)

    def dot(a, b):
        return jnp.dot(a, b, preferred_element_type=jnp.float32)

    def gelu(c):
        c = lax.reduce_precision(c, 8, 7)
        return jax.nn.gelu(c, approximate=True).astype(jnp.bfloat16)

    def local_mlp(x, w1, w2):
        cy, cx = lax.axis_index('cy'), lax.axis_index('cx')
        rows, depth = x.shape
        half = w1.shape[1] // 2
        unit = half // sum(CHUNKS)
        starts = [unit * sum(CHUNKS[:j]) for j in range(len(CHUNKS))]
        sizes = [unit * c for c in CHUNKS]

        def columns(side, j):
            return lax.dynamic_slice(w1, (0, side * half + starts[j]), (depth, sizes[j]))

        x_o = to_x(x)
        w1_recv = []
        for j in range(len(CHUNKS)):
            piece = columns(1 - cy, j)
            if j:
                piece = after(piece, x_o if j == 1 else w1_recv[j - 2])
            w1_recv.append(to_x(piece))

        x_y = to_y(x)
        xo_y = to_y(x_o)

        def both(v):
            return after(jnp.concatenate([v, to_core(v)], 0))

        rows_own = {'A': both(x), 'B': both(x_y)}
        rows_oth = {'A': both(x_o), 'B': both(xo_y)}

        part_up = {'A': [], 'B': []}
        for name in 'AB':
            for j in range(len(CHUNKS)):
                part_up[name].append(after(dot(rows_own[name], columns(cy, j))))
        hid = {'A': [], 'B': []}
        for j in range(len(CHUNKS)):
            for name in 'BA':
                c = dot(rows_oth[name], w1_recv[j]) + part_up[name][j]
                hid[name].append(gelu(c))

        w2_o = to_core(w2)

        def down(quarters):
            width = w2.shape[1]
            buf = jnp.zeros((2 * half, 2 * width), w2.dtype)
            for r, (pcx, pcy) in enumerate(quarters):
                for c, w in enumerate((w2, w2_o)):
                    piece = lax.dynamic_slice(w, (pcx * (2 * half) + pcy * half, 0), (half, width))
                    buf = lax.dynamic_update_slice(buf, piece, (r * half, c * width))
            return after(buf)

        w2_own = down(((cx, cy), (1 - cx, cy)))
        w2_recv = down(((cx, 1 - cy), (1 - cx, 1 - cy)))

        blocks = []
        for name, shares in (('B', B_BLOCKS), ('A', A_BLOCKS)):
            step = rows // sum(shares)
            blocks += [(name, step * sum(shares[:k]), step * s) for k, s in enumerate(shares)]

        h_own, h_recv, arrived = [], [], []
        for i, (name, start, size) in enumerate(blocks):
            def part(chunks, base):
                return cat([hid[name][j][base + start:base + start + size] for j in chunks], 1)

            every = list(range(len(CHUNKS)))
            groups = [every[:-1], every[-1:]] if i == 0 else [every]
            own, core, xs, ds = [], [], [], []
            for chunks in groups:
                mine, theirs = part(chunks, 0), part(chunks, rows)
                if i >= 2:
                    mine, theirs = after((mine, theirs), arrived[i - 2])
                xs.append(to_x(mine))
                ds.append(to_diag(theirs))
                core.append(to_core(theirs))
                own.append(mine)
            arrived.append((xs[-1], ds[-1]))
            h_own.append(after(jnp.concatenate([*own, *core], 1)))
            h_recv.append(after(jnp.concatenate([*xs, *ds], 1)))

        from_y = []
        out = jnp.zeros(x.shape, x.dtype)
        for i, (name, start, size) in enumerate(blocks):
            z_own = after(dot(h_own[i], w2_own))
            if name == 'B':
                z = dot(h_recv[i], w2_recv) + z_own
                from_y.append((start, to_y(z)))
            else:
                base, rest = next((b, v) for b, v in reversed(from_y) if b <= start)
                z = (dot(h_recv[i], w2_recv) + z_own) + rest[start - base:start - base + size]
                z = z.astype(x.dtype)
                z = jnp.where(cx == 0, z, jnp.roll(z, depth // 2, 1))
                out = lax.dynamic_update_slice(out, z, (start, 0))
        return out

    return jax.shard_map(local_mlp, mesh=mesh, in_specs=(data_spec, up_spec, down_spec), out_specs=data_spec, check_vma=False)
```

```python
import jax
import jax.numpy as jnp
from jax import lax
from jax.sharding import PartitionSpec as P


CHUNKS = (2, 2, 2, 1)
B_BLOCKS = (2, 2)
A_BLOCKS = (2, 1, 1)


def solution(mesh):
    data_spec = P(('dp', 'cx', 'cz'), 'cy')
    up_spec = P('cy', ('cz', 'cx'))
    down_spec = P('cz', ('cy', 'cx'))
    swap = [(0, 1), (1, 0)]

    def to_core(v):
        return lax.ppermute(v, 'cx', swap)

    def to_y(v):
        return lax.ppermute(v, 'cz', swap)

    def to_x(v):
        return lax.ppermute(v, 'cy', swap)

    def to_diag(v):
        return lax.ppermute(v, ('cy', 'cx'), [(0, 3), (1, 2), (2, 1), (3, 0)])

    def after(v, *deps):
        return lax.optimization_barrier((v, *deps))[0]

    def cat(pieces, axis):
        return pieces[0] if len(pieces) == 1 else jnp.concatenate(pieces, axis)

    def dot(a, b):
        return jnp.dot(a, b, preferred_element_type=jnp.float32)

    def gelu(c):
        c = lax.reduce_precision(c, 8, 7)
        return jax.nn.gelu(c, approximate=True).astype(jnp.bfloat16)

    def local_mlp(x, w1, w2):
        cy, cx = lax.axis_index('cy'), lax.axis_index('cx')
        rows, depth = x.shape
        half = w1.shape[1] // 2
        unit = half // sum(CHUNKS)
        starts = [unit * sum(CHUNKS[:j]) for j in range(len(CHUNKS))]
        sizes = [unit * c for c in CHUNKS]

        def columns(side, j):
            return lax.dynamic_slice(w1, (0, side * half + starts[j]), (depth, sizes[j]))

        x_o = to_x(x)
        w1_recv = []
        for j in range(len(CHUNKS)):
            piece = columns(1 - cy, j)
            if j:
                piece = after(piece, x_o if j == 1 else w1_recv[j - 2])
            w1_recv.append(to_x(piece))

        x_y = to_y(x)
        xo_y = to_y(x_o)

        def both(v):
            return after(jnp.concatenate([v, to_core(v)], 0))

        x_own = both(x)
        rows_own = {'A': x_own, 'B': both(x_y)}
        rows_oth = {'A': both(x_o), 'B': both(xo_y)}

        part_up = {'A': [], 'B': []}
        for name in 'AB':
            for j in range(len(CHUNKS)):
                part_up[name].append(after(dot(rows_own[name], columns(cy, j))))
        hid = {'A': [], 'B': []}
        for j in range(len(CHUNKS)):
            for name in 'BA':
                c = dot(rows_oth[name], w1_recv[j]) + part_up[name][j]
                hid[name].append(gelu(c))

        w2_o = to_core(w2)

        def down(quarters):
            width = w2.shape[1]
            buf = jnp.zeros((2 * half, 2 * width), w2.dtype)
            for r, (pcx, pcy) in enumerate(quarters):
                for c, w in enumerate((w2, w2_o)):
                    piece = lax.dynamic_slice(w, (pcx * (2 * half) + pcy * half, 0), (half, width))
                    buf = lax.dynamic_update_slice(buf, piece, (r * half, c * width))
            return after(buf)

        w2_own = down(((cx, cy), (1 - cx, cy)))
        w2_recv = down(((cx, 1 - cy), (1 - cx, 1 - cy)))

        blocks = []
        for name, shares in (('B', B_BLOCKS), ('A', A_BLOCKS)):
            step = rows // sum(shares)
            blocks += [(name, step * sum(shares[:k]), step * s) for k, s in enumerate(shares)]

        every = list(range(len(CHUNKS)))
        final = len(blocks) - 1
        h_own, h_recv, arrived = [], [], []
        for i, (name, start, size) in enumerate(blocks):
            def part(chunks, base):
                return cat([hid[name][j][base + start:base + start + size] for j in chunks], 1)

            x_groups = d_groups = [every]
            if i == 0:
                x_groups = d_groups = [every[:-1], every[-1:]]
            if i == final:
                x_groups = [every[:2], every[2:]]

            def send(groups, base, *movers):
                sent, got = [], [[] for _ in movers]
                for chunks in groups:
                    piece = part(chunks, base)
                    sent.append(piece)
                    held = after(piece, arrived[i - 2]) if i >= 2 else piece
                    for k, (mover, source) in enumerate(movers):
                        got[k].append(mover(held if source else piece))
                return sent, got

            own, (xs,) = send(x_groups, 0, (to_x, True))
            _, (ds, core) = send(d_groups, rows, (to_diag, True), (to_core, False))
            arrived.append((xs[-1], ds[-1]))
            h_own.append(after(jnp.concatenate([*own, *core], 1)))
            h_recv.append((xs, ds, x_groups))

        from_y = []
        out = jnp.zeros(x.shape, x.dtype)
        for i, (name, start, size) in enumerate(blocks):
            xs, ds, x_groups = h_recv[i]
            z_own = after(dot(h_own[i], w2_own))
            if i != final:
                recv = after(jnp.concatenate([*xs, *ds], 1))
                z = dot(recv, w2_recv) + z_own
            if name == 'B':
                from_y.append((start, to_y(z)))
                continue
            base, rest = next((b, v) for b, v in reversed(from_y) if b <= start)
            rest = rest[start - base:start - base + size]
            if i != final:
                z = (z + rest).astype(x.dtype)
            else:
                z = after((dot(ds[0], w2_recv[half:]) + z_own) + rest)
                for g, (piece, chunks) in enumerate(zip(xs, x_groups)):
                    row = starts[chunks[0]]
                    z = dot(piece, w2_recv[row:row + piece.shape[1]]) + z
                    z = after(z) if g == 0 else z.astype(x.dtype)
            z = jnp.where(cx == 0, z, jnp.roll(z, depth // 2, 1))
            out = lax.dynamic_update_slice(out, z, (start, 0))
        return out

    return jax.shard_map(local_mlp, mesh=mesh, in_specs=(data_spec, up_spec, down_spec), out_specs=data_spec, check_vma=False)
```

```python
import jax
import jax.numpy as jnp
from jax import lax
from jax.experimental import pallas as pl
from jax.experimental.pallas import tpu as pltpu
from jax.sharding import PartitionSpec as P


CHUNKS = (2, 2, 2, 1)
B_BLOCKS = (2, 2)
A_BLOCKS = (2, 1, 1)
TAIL_TILES = 8


def tail_dot(shift, h, w, w_blocks, terms, out=None, out_row=0):
    size, width = h.shape[0], w.shape[1]
    tile = width // TAIL_TILES
    rows = h.shape[1] // len(w_blocks)
    n_w, n_t = len(w_blocks), len(terms)

    def kernel(shift_ref, h_ref, *refs):
        acc = refs[n_w][...]
        for t in refs[n_w + 1:n_w + n_t]:
            acc = acc + t[...]
        for k in range(n_w):
            acc = acc + jnp.dot(h_ref[:, k * rows:(k + 1) * rows], refs[k][...], preferred_element_type=jnp.float32)
        refs[-1][...] = acc.astype(refs[-1].dtype)

    in_specs = [pl.BlockSpec((size, h.shape[1]), lambda n, c: (0, 0))]
    in_specs += [pl.BlockSpec((rows, tile), lambda n, c, b=b: (b, n)) for b in w_blocks]
    in_specs += [pl.BlockSpec((size, tile), lambda n, c, b=b: (b, n)) for _, b in terms]
    args = [h, *([w] * n_w), *(t for t, _ in terms)]
    if out is None:
        out_shape = jax.ShapeDtypeStruct((size, width), jnp.float32)
        out_spec, aliases = pl.BlockSpec((size, tile), lambda n, c: (0, n)), {}
    else:
        in_specs.append(pl.BlockSpec(memory_space=pl.ANY))
        args.append(out)
        out_shape = jax.ShapeDtypeStruct(out.shape, out.dtype)
        out_spec = pl.BlockSpec((size, tile), lambda n, c: (out_row // size, lax.rem(n + c[0], TAIL_TILES)))
        aliases = {len(args): 0}
    return pl.pallas_call(
        kernel,
        grid_spec=pltpu.PrefetchScalarGridSpec(
            num_scalar_prefetch=1, grid=(TAIL_TILES,), in_specs=in_specs, out_specs=out_spec),
        out_shape=out_shape,
        input_output_aliases=aliases,
        cost_estimate=pl.CostEstimate(
            flops=2 * size * h.shape[1] * width, bytes_accessed=2 * h.shape[1] * width, transcendentals=0),
    )(shift, *args)


def solution(mesh):
    data_spec = P(('dp', 'cx', 'cz'), 'cy')
    up_spec = P('cy', ('cz', 'cx'))
    down_spec = P('cz', ('cy', 'cx'))
    swap = [(0, 1), (1, 0)]

    def to_core(v):
        return lax.ppermute(v, 'cx', swap)

    def to_y(v):
        return lax.ppermute(v, 'cz', swap)

    def to_x(v):
        return lax.ppermute(v, 'cy', swap)

    def to_diag(v):
        return lax.ppermute(v, ('cy', 'cx'), [(0, 3), (1, 2), (2, 1), (3, 0)])

    def after(v, *deps):
        return lax.optimization_barrier((v, *deps))[0]

    def cat(pieces, axis):
        return pieces[0] if len(pieces) == 1 else jnp.concatenate(pieces, axis)

    def dot(a, b):
        return jnp.dot(a, b, preferred_element_type=jnp.float32)

    def gelu(c):
        c = lax.reduce_precision(c, 8, 7)
        return jax.nn.gelu(c, approximate=True).astype(jnp.bfloat16)

    def local_mlp(x, w1, w2):
        cy, cx = lax.axis_index('cy'), lax.axis_index('cx')
        rows, depth = x.shape
        half = w1.shape[1] // 2
        unit = half // sum(CHUNKS)
        starts = [unit * sum(CHUNKS[:j]) for j in range(len(CHUNKS))]
        sizes = [unit * c for c in CHUNKS]

        def columns(side, j):
            return lax.dynamic_slice(w1, (0, side * half + starts[j]), (depth, sizes[j]))

        x_o = to_x(x)
        w1_recv = []
        for j in range(len(CHUNKS)):
            piece = columns(1 - cy, j)
            if j:
                piece = after(piece, x_o if j == 1 else w1_recv[j - 2])
            w1_recv.append(to_x(piece))

        x_y = to_y(x)
        xo_y = to_y(x_o)

        def both(v):
            return after(jnp.concatenate([v, to_core(v)], 0))

        x_own = both(x)
        rows_own = {'A': x_own, 'B': both(x_y)}
        rows_oth = {'A': both(x_o), 'B': both(xo_y)}

        part_up = {'A': [], 'B': []}
        for name in 'AB':
            for j in range(len(CHUNKS)):
                part_up[name].append(after(dot(rows_own[name], columns(cy, j))))
        hid = {'A': [], 'B': []}
        for j in range(len(CHUNKS)):
            for name in 'BA':
                c = dot(rows_oth[name], w1_recv[j]) + part_up[name][j]
                hid[name].append(gelu(c))

        w2_o = to_core(w2)

        def down(quarters):
            width = w2.shape[1]
            buf = jnp.zeros((2 * half, 2 * width), w2.dtype)
            for r, (pcx, pcy) in enumerate(quarters):
                for c, w in enumerate((w2, w2_o)):
                    piece = lax.dynamic_slice(w, (pcx * (2 * half) + pcy * half, 0), (half, width))
                    buf = lax.dynamic_update_slice(buf, piece, (r * half, c * width))
            return after(buf)

        w2_own = down(((cx, cy), (1 - cx, cy)))
        w2_recv = down(((cx, 1 - cy), (1 - cx, 1 - cy)))

        blocks = []
        for name, shares in (('B', B_BLOCKS), ('A', A_BLOCKS)):
            step = rows // sum(shares)
            blocks += [(name, step * sum(shares[:k]), step * s) for k, s in enumerate(shares)]

        every = list(range(len(CHUNKS)))
        final = len(blocks) - 1
        h_own, h_recv, arrived = [], [], []
        for i, (name, start, size) in enumerate(blocks):
            def part(chunks, base):
                return cat([hid[name][j][base + start:base + start + size] for j in chunks], 1)

            x_groups = d_groups = [every]
            if i == 0:
                x_groups = d_groups = [every[:-1], every[-1:]]
            if i == final:
                x_groups = [every[:2], every[2:]]

            def send(groups, base, *movers):
                sent, got = [], [[] for _ in movers]
                for chunks in groups:
                    piece = part(chunks, base)
                    sent.append(piece)
                    held = after(piece, arrived[i - 2]) if i >= 2 else piece
                    for k, (mover, source) in enumerate(movers):
                        got[k].append(mover(held if source else piece))
                return sent, got

            own, (xs,) = send(x_groups, 0, (to_x, True))
            _, (ds, core) = send(d_groups, rows, (to_diag, True), (to_core, False))
            arrived.append((xs[-1], ds[-1]))
            h_own.append(after(jnp.concatenate([*own, *core], 1)))
            h_recv.append((xs, ds, x_groups))

        from_y = []
        out = jnp.zeros(x.shape, x.dtype)
        for i, (name, start, size) in enumerate(blocks):
            xs, ds, x_groups = h_recv[i]
            z_own = after(dot(h_own[i], w2_own))
            if i != final:
                recv = after(jnp.concatenate([*xs, *ds], 1))
                z = dot(recv, w2_recv) + z_own
            if name == 'B':
                from_y.append((start, to_y(z)))
                continue
            base, rest = next((b, v) for b, v in reversed(from_y) if b <= start)
            if i != final:
                z = z + rest[start - base:start - base + size]
                z = z.astype(x.dtype)
                z = jnp.where(cx == 0, z, jnp.roll(z, depth // 2, 1))
                out = lax.dynamic_update_slice(out, z, (start, 0))
                continue
            shift = jnp.full((1,), cx * (TAIL_TILES // 2), jnp.int32)
            z = tail_dot(shift, ds[0], w2_recv, [1], [(z_own, 0), (rest, (start - base) // size)])
            for g, (piece, chunks) in enumerate(zip(xs, x_groups)):
                first, count = starts[chunks[0]] // unit, piece.shape[1] // unit
                if g == 0:
                    z = tail_dot(shift, piece, w2_recv, list(range(first, first + count)), [(z, 0)])
                else:
                    out = tail_dot(shift, piece, w2_recv, list(range(first, first + count)), [(z, 0)], out, start)
        return out

    return jax.shard_map(local_mlp, mesh=mesh, in_specs=(data_spec, up_spec, down_spec), out_specs=data_spec, check_vma=False)
```
